32 devices in a mesh: dp: 2 (over x), expert: 16 (over z, y, core).
Axes of the slice: x: 2, y: 2, z: 4, core: 2. Of those that a mesh axis runs over, the one named last changes fastest.
Arguments:
- tokens: bfloat16 [4096, 2880], P('expert'), may hold values from -2 to 2
- segment_ids: int32 [4096], P('expert'), may hold values from 0 to 31, never falling along the last dimension, each value on 1 to 512 neighbouring positions
- expert_ids: int32 [4096, 4], P('expert'), may hold values from 0 to 15, as said below
- attn_gain: float32 [2880], replicated, may hold values from 0.1 to 1.9
- sinks: float32 [32], P('dp'), may hold values from 2 to 5
- qkv_master: float32 [2560, 2880], P(('dp', 'expert')), may hold values from -0.109375 to 0.109375
- qkv_mom: float32 [2560, 2880], P(('dp', 'expert')), may hold values from -0.006 to 0.006
- qkv_var: float32 [2560, 2880], P(('dp', 'expert')), may hold values from 1e-08 to 1e-06
- qkv_grad: float32 [2560, 2880], P(('dp', 'expert')), may hold values from -0.06 to 0.06
- o_master: float32 [2048, 2880], P(('dp', 'expert')), may hold values from -0.125 to 0.125
- o_mom: float32 [2048, 2880], P(('dp', 'expert')), may hold values from -0.006 to 0.006
- o_var: float32 [2048, 2880], P(('dp', 'expert')), may hold values from 1e-08 to 1e-06
- o_grad: float32 [2048, 2880], P(('dp', 'expert')), may hold values from -0.06 to 0.06
- router_weight: bfloat16 [2880, 16], replicated, may hold values from -0.109375 to 0.109375
- router_bias: float32 [16], replicated, may hold values from -4 to 4
- mlp_gain: float32 [2880], replicated, may hold values from 0.1 to 1.9
Outputs:
- dispatched: bfloat16 [16, 16, 2, 64, 2880], P('expert', None, 'dp')
- gate_slots: bfloat16 [16, 16, 2, 64], P('expert', None, 'dp')
The draws below stay inside these ranges and needn't reach their ends.
Inputs may be any that keep to these rules, and one draw needn't show every extreme that they name: `expert_ids`: each row names 4 different experts. In each aligned block of 128 rows no expert is named more than 64 times, and one expert, the same in every block of a draw, is named exactly 64 times in every block.
All inputs are finite; a program needn't handle non-finite values.
Results may differ from the reference program's by a relative error of at most 0.012.
The reference program's roundings to bfloat16 on the way count: a program that leaves them out, or rounds other values in their place, can miss the bound.
Values may be sent and summed in bfloat16 or wider, within the bound.
No kernel may reach another device: no remote copies, remote signals or barrier semaphores. Data moves between devices by JAX's collectives and lax.ppermute only.
A program may use at most 128 MiB of HBM per device.

```python
import math
import jax
import jax.numpy as jnp
import numpy as np
from jax import lax

D = 2880
HEADS = 32
KV_HEADS = 4
HEAD_DIM = 64
WINDOW = 128
TOPK = 4
TOK_DEV = 256
EXPERTS = 16
TOKENS = 4096
BLOCK = 128
CAP = 64
QKV_ROWS = 2560
O_ROWS = 2048
N_DP = 2
N_EXPERT = 16


def draw_expert_ids(key, part):
    blocks = TOKENS // BLOCK
    pair_half = EXPERTS // 2
    base_key = jax.random.fold_in(key, 11)
    chosen = jax.random.randint(jax.random.fold_in(base_key, 1), (), 0, EXPERTS).astype(jnp.int32)

    def one_block(index):
        block_key = jax.random.fold_in(base_key, index + 7)
        ordering = jax.random.permutation(jax.random.fold_in(block_key, 1), EXPERTS).astype(jnp.int32)
        shares = jax.random.randint(jax.random.fold_in(block_key, 2), (pair_half,), 0, CAP + 1).astype(jnp.int32)
        where_pos = jnp.argmax(ordering == chosen).astype(jnp.int32)
        pair_pos = where_pos % pair_half
        forced = jnp.where(where_pos < pair_half, CAP, 0).astype(jnp.int32)
        shares = jnp.where(jnp.arange(pair_half, dtype=jnp.int32) == pair_pos, forced, shares)
        counts = jnp.zeros((EXPERTS,), jnp.int32).at[ordering].set(jnp.concatenate([shares, CAP - shares]))
        bounds = jnp.cumsum(counts)
        listing = jnp.searchsorted(bounds, jnp.arange(BLOCK * TOPK, dtype=jnp.int32), side='right').astype(jnp.int32)
        layout = listing.reshape(TOPK, BLOCK).T
        shuffle = jax.random.permutation(jax.random.fold_in(block_key, 3), BLOCK)
        return layout[shuffle]
    return jax.vmap(one_block)(jnp.arange(blocks, dtype=jnp.int32)).reshape(TOKENS, TOPK).astype(jnp.int32)


def block_levels(own_key, extent, cuts, least, top_value):
    factor_of = 1.0
    for dim, shards_of in cuts:
        heights = jax.random.uniform(jax.random.fold_in(jax.random.fold_in(own_key, 6), dim), (shards_of,), jnp.float32, least / len(cuts), top_value / len(cuts))
        factor_of = factor_of * jnp.repeat(jnp.exp(heights), extent[dim] // shards_of).reshape((-1,) + (1,) * (len(extent) - 1 - dim))
    return factor_of


def split_up(amount, total, reach, lean):
    weights = [(1 << 20) // math.isqrt(standing ** lean) + 1 for standing in range(2, amount + 1)]
    spare, given = total - reach - (amount - 1), [1] * (amount - 1)
    while spare > 0:
        candidates = [i for i in range(amount - 1) if given[i] < reach]
        mass, left = sum([weights[i] for i in candidates]), spare
        for i in candidates:
            extra = min(reach - given[i], max(1, left * weights[i] // mass), spare)
            given[i] = given[i] + extra
            spare = spare - extra
    return np.array([reach] + given)


def ragged_sizes(own_key, count, total, bound, skew):
    if count == 2:
        one = jax.random.randint(own_key, (), max(1, total - bound), min(bound, total - 1) + 1)
        return jnp.stack([one, total - one])
    tallies = jnp.asarray(split_up(count, total, bound, skew), jnp.int32)
    couples = (count - 1) // 2
    donor, sink = tallies[1:1 + 2 * couples:2], tallies[2:2 + 2 * couples:2]
    room = jnp.minimum(donor - 1, bound - sink)
    shifted = jax.random.randint(jax.random.fold_in(own_key, 1), (couples,), 0, 1 << 20) % (room + 1)
    tallies = tallies.at[1:1 + 2 * couples:2].set(donor - shifted).at[2:2 + 2 * couples:2].set(sink + shifted)
    return tallies[jax.random.permutation(jax.random.fold_in(own_key, 2), count)]


def noise(rng, dims, deviation, bound, split=(), kind=jnp.bfloat16):
    array = deviation * jax.random.normal(rng, dims, jnp.float32)
    if split:
        array = array * block_levels(rng, dims, split, -0.22, 0.18)
    return jnp.clip(array, -bound, bound).astype(kind)


def setup_inputs(seed: int = 0) -> dict:
    key_list = jax.random.split(jax.random.key(seed), 17)
    tokens = noise(key_list[0], (TOKENS, D), 0.3, 2.0, ((0, 16),))
    segment_ids = jnp.searchsorted(jnp.cumsum(ragged_sizes(key_list[1], TOKENS // 128, TOKENS, 512, 1)), jnp.arange(TOKENS), side="right").astype(jnp.int32)
    expert_ids = draw_expert_ids(jax.random.fold_in(key_list[16], 71), 0)
    attn_gain = jnp.clip(1.0 + 0.18 * jax.random.normal(key_list[3], (D,), jnp.float32), 0.1, 1.9)
    sinks = jnp.clip(2.0 + 3.0 * jax.random.uniform(key_list[4], (HEADS,), jnp.float32) ** block_levels(key_list[4], (HEADS,), ((0, 2),), -0.2, 0.2), 2.0, 5.0)
    qkv_master = noise(key_list[5], (QKV_ROWS, D), D ** -0.5, 0.109375, ((0, 32),), jnp.float32)
    qkv_mom = noise(key_list[6], (QKV_ROWS, D), 0.001, 0.006, ((0, 32),), jnp.float32)
    qkv_var = jnp.clip(jnp.exp(math.log(9.999999974752427e-07) - 4.6051702 * jax.random.uniform(key_list[7], (QKV_ROWS, D), jnp.float32) ** block_levels(key_list[7], (QKV_ROWS, D), ((0, 32),), -0.2, 0.2)), 9.99999993922529e-09, 9.999999974752427e-07)
    qkv_grad = noise(key_list[8], (QKV_ROWS, D), 0.01, 0.06, ((0, 32),), jnp.float32)
    o_master = noise(key_list[9], (O_ROWS, D), O_ROWS ** -0.5, 0.125, ((0, 32),), jnp.float32)
    o_mom = noise(key_list[10], (O_ROWS, D), 0.001, 0.006, ((0, 32),), jnp.float32)
    o_var = jnp.clip(jnp.exp(math.log(9.999999974752427e-07) - 4.6051702 * jax.random.uniform(key_list[11], (O_ROWS, D), jnp.float32) ** block_levels(key_list[11], (O_ROWS, D), ((0, 32),), -0.2, 0.2)), 9.99999993922529e-09, 9.999999974752427e-07)
    o_grad = noise(key_list[12], (O_ROWS, D), 0.01, 0.06, ((0, 32),), jnp.float32)
    router_weight = noise(key_list[13], (D, EXPERTS), D ** -0.5, 0.109375)
    router_bias = noise(key_list[14], (EXPERTS,), 1.0, 4.0, (), jnp.float32)
    mlp_gain = jnp.clip(1.0 + 0.18 * jax.random.normal(key_list[15], (D,), jnp.float32), 0.1, 1.9)
    return dict(tokens=tokens, segment_ids=segment_ids, expert_ids=expert_ids, attn_gain=attn_gain, sinks=sinks, qkv_master=qkv_master, qkv_mom=qkv_mom, qkv_var=qkv_var, qkv_grad=qkv_grad, o_master=o_master, o_mom=o_mom, o_var=o_var, o_grad=o_grad, router_weight=router_weight, router_bias=router_bias, mlp_gain=mlp_gain)


beta_one = 0.9
beta_two = 0.999
adam_step = 100
learn_rate = 0.02
adam_eps = 1e-08
norm_eps = 1e-05
rope_base = 150000.0
contract_rows = (((1,), (1,)), ((), ()))

def adam_weights(master, moment, second_mom, gradient):
    moment_new = beta_one * moment + (1.0 - beta_one) * gradient
    second_new = beta_two * second_mom + (1.0 - beta_two) * gradient * gradient
    fix_one = 1.0 - beta_one ** adam_step
    fix_two = 1.0 - beta_two ** adam_step
    update = moment_new / fix_one / (jnp.sqrt(second_new / fix_two) + adam_eps)
    return (master - learn_rate * update).astype(jnp.bfloat16)

def rms_scale(values, gain_vec):
    mean_sq = lax.optimization_barrier(jnp.mean(values * values, axis=-1, keepdims=True))
    return values * lax.rsqrt(mean_sq + norm_eps) * gain_vec

def rotate(values, positions):
    half_dim = values.shape[-1] // 2
    frequency = rope_base ** (-(jnp.arange(half_dim).astype(jnp.float32) * 2.0) / values.shape[-1])
    angles = positions[:, None] * frequency[None, :]
    cosine = jnp.cos(angles)[:, None, :]
    sine_vals = jnp.sin(angles)[:, None, :]
    first_half = values[..., :half_dim]
    second_half = values[..., half_dim:]
    return jnp.concatenate([first_half * cosine - second_half * sine_vals, second_half * cosine + first_half * sine_vals], axis=-1)

def attention(queries, key_rows, value_rows, segments, sink_logits):
    row_count = queries.shape[0]
    scale = queries.shape[-1] ** (-0.5)
    scores = jnp.einsum('tgrd,ugd->grtu', queries.astype(jnp.float32), key_rows.astype(jnp.float32)) * scale
    position = jnp.arange(row_count, dtype=jnp.int32)
    offset = position[:, None] - position[None, :]
    allowed = (segments[:, None] == segments[None, :]) & (offset >= 0) & (offset < WINDOW)
    weights = jnp.where(allowed, jnp.exp(scores), 0.0)
    sink_terms = jnp.exp(sink_logits).reshape(key_rows.shape[1], -1)[:, :, None]
    running = sink_terms + lax.optimization_barrier(jnp.sum(weights, axis=-1))
    attn_probs = (weights / running[..., None]).astype(jnp.bfloat16)
    attended = jnp.einsum('grtu,ugd->tgrd', attn_probs.astype(jnp.float32), value_rows.astype(jnp.float32))
    return attended.astype(jnp.bfloat16).reshape(row_count, -1)

def gate_values(logits, choices, experts):
    picked = choices[:, :, None] == jnp.arange(experts, dtype=jnp.int32)[None, None, :]
    chosen = lax.optimization_barrier(jnp.sum(jnp.where(picked, logits[:, None, :], 0.0), axis=-1))
    raised = jnp.exp(chosen)
    return raised / lax.optimization_barrier(jnp.sum(raised, axis=-1, keepdims=True))

def slot_targets(choices, capacity, experts):
    flat_ids = choices.reshape(-1).astype(jnp.int32)
    onehot = (flat_ids[:, None] == jnp.arange(experts, dtype=jnp.int32)[None, :]).astype(jnp.int32)
    earlier = jnp.cumsum(onehot, axis=0) - onehot
    slot_index = lax.optimization_barrier(jnp.sum(earlier * onehot, axis=1)).astype(jnp.int32)
    return flat_ids * capacity + slot_index

def reference(tokens, segment_ids, expert_ids, attn_gain, sinks, qkv_master, qkv_mom, qkv_var, qkv_grad, o_master, o_mom, o_var, o_grad, router_weight, router_bias, mlp_gain):
    qkv_weight = adam_weights(qkv_master, qkv_mom, qkv_var, qkv_grad)
    o_weight = adam_weights(o_master, o_mom, o_var, o_grad)
    group_rows = QKV_ROWS // N_DP
    q_rows = HEADS // N_DP * HEAD_DIM
    kv_rows = KV_HEADS // N_DP * HEAD_DIM
    repeat_count = HEADS // KV_HEADS
    positions = jnp.arange(TOK_DEV).astype(jnp.float32)

    def per_pack(pack_data):
        rows, segments, choices = pack_data
        normed = rms_scale(rows.astype(jnp.float32), attn_gain).astype(jnp.bfloat16)
        projected = lax.dot_general(normed, qkv_weight, contract_rows, preferred_element_type=jnp.float32)
        projected = projected.reshape(TOK_DEV, N_DP, group_rows)
        queries = rotate(projected[:, :, :q_rows].reshape(TOK_DEV, HEADS, HEAD_DIM), positions).astype(jnp.bfloat16)
        queries = queries.reshape(TOK_DEV, KV_HEADS, repeat_count, HEAD_DIM)
        key_rows = rotate(projected[:, :, q_rows:q_rows + kv_rows].reshape(TOK_DEV, KV_HEADS, HEAD_DIM), positions).astype(jnp.bfloat16)
        value_rows = projected[:, :, q_rows + kv_rows:].reshape(TOK_DEV, KV_HEADS, HEAD_DIM).astype(jnp.bfloat16)
        attended = attention(queries, key_rows, value_rows, segments, sinks)
        residual = rows.astype(jnp.float32) + jnp.dot(attended, o_weight, preferred_element_type=jnp.float32)
        moe_all = rms_scale(residual, mlp_gain).astype(jnp.bfloat16)
        payloads = []
        gate_lists = []
        for group_num in range(N_DP):
            row_start = group_num * BLOCK
            moe_in = moe_all[row_start:row_start + BLOCK]
            block_ids = choices[row_start:row_start + BLOCK]
            logits = jnp.dot(moe_in, router_weight, preferred_element_type=jnp.float32) + router_bias
            gate_vals = gate_values(logits, block_ids, EXPERTS)
            target = slot_targets(block_ids, CAP, EXPERTS)
            source_row = jnp.arange(BLOCK * TOPK, dtype=jnp.int32) // TOPK
            payload = jnp.zeros((EXPERTS * CAP, D), jnp.bfloat16).at[target].set(moe_in[source_row])
            slot_gates = jnp.zeros((EXPERTS * CAP,), jnp.bfloat16).at[target].set(gate_vals.reshape(-1).astype(jnp.bfloat16))
            payloads.append(payload.reshape(EXPERTS, CAP, D))
            gate_lists.append(slot_gates.reshape(EXPERTS, CAP))
        return (jnp.stack(payloads), jnp.stack(gate_lists))
    packed = (tokens.reshape(N_EXPERT, TOK_DEV, D), segment_ids.reshape(N_EXPERT, TOK_DEV), expert_ids.reshape(N_EXPERT, TOK_DEV, TOPK))
    payload_all, gates_all = lax.map(per_pack, packed)
    dispatched = jnp.transpose(payload_all, (2, 0, 1, 3, 4))
    gate_slots = jnp.transpose(gates_all, (2, 0, 1, 3))
    return (dispatched, gate_slots)
```

```python
import jax
import jax.numpy as jnp
from jax import lax
from jax.sharding import PartitionSpec as P

HEADS = 32
KV_HEADS = 4
HEAD_DIM = 64
WINDOW = 128


beta_one = 0.9
beta_two = 0.999
adam_step = 100
learn_rate = 0.02
adam_eps = 1e-08
norm_eps = 1e-05
rope_base = 150000.0
contract_rows = (((1,), (1,)), ((), ()))
ring_limit = 16


def adam_weights(master, moment, second_mom, gradient):
    moment_new = beta_one * moment + (1.0 - beta_one) * gradient
    second_new = beta_two * second_mom + (1.0 - beta_two) * gradient * gradient
    fix_one = 1.0 - beta_one**adam_step
    fix_two = 1.0 - beta_two**adam_step
    update = moment_new / fix_one / (jnp.sqrt(second_new / fix_two) + adam_eps)
    return (master - learn_rate * update).astype(jnp.bfloat16)


def rms_scale(values, gain_vec):
    mean_sq = jnp.mean(values * values, axis=-1, keepdims=True)
    return values * lax.rsqrt(mean_sq + norm_eps) * gain_vec


def rotate(values, positions):
    half_dim = values.shape[-1] // 2
    frequency = rope_base ** (-(jnp.arange(half_dim).astype(jnp.float32) * 2.0) / values.shape[-1])
    angles = positions[:, None] * frequency[None, :]
    cosine = jnp.cos(angles)[:, None, :]
    sine_vals = jnp.sin(angles)[:, None, :]
    first_half = values[..., :half_dim]
    second_half = values[..., half_dim:]
    return jnp.concatenate(
        [
            first_half * cosine - second_half * sine_vals,
            second_half * cosine + first_half * sine_vals,
        ],
        axis=-1,
    )


def attention(queries, key_rows, value_rows, segments, sink_logits):
    row_count = queries.shape[0]
    scale = queries.shape[-1] ** (-0.5)
    scores = (
        jnp.einsum("tgrd,ugd->grtu", queries, key_rows, preferred_element_type=jnp.float32) * scale
    )
    position = jnp.arange(row_count, dtype=jnp.int32)
    offset = position[:, None] - position[None, :]
    allowed = (segments[:, None] == segments[None, :]) & (offset >= 0) & (offset < WINDOW)
    weights = jnp.where(allowed, jnp.exp(scores), 0.0)
    sink_terms = jnp.exp(sink_logits).reshape(key_rows.shape[1], -1)[:, :, None]
    running = sink_terms + jnp.sum(weights, axis=-1)
    attn_probs = (weights / running[..., None]).astype(jnp.bfloat16)
    attended = jnp.einsum(
        "grtu,ugd->tgrd", attn_probs, value_rows, preferred_element_type=jnp.float32
    )
    return attended.astype(jnp.bfloat16).reshape(row_count, -1)


def gate_values(logits, choices, experts):
    picked = choices[:, :, None] == jnp.arange(experts, dtype=jnp.int32)[None, None, :]
    chosen = jnp.sum(jnp.where(picked, logits[:, None, :], 0.0), axis=-1)
    raised = jnp.exp(chosen)
    return raised / jnp.sum(raised, axis=-1, keepdims=True)


def slot_numbers(choices, experts):
    flat_ids = choices.reshape(-1)
    onehot = (flat_ids[:, None] == jnp.arange(experts, dtype=jnp.int32)[None, :]).astype(jnp.int32)
    earlier = jnp.cumsum(onehot, axis=0) - onehot
    return jnp.sum(earlier * onehot, axis=1).reshape(choices.shape)


def use_ring(members):
    return members % 4 == 0 and members <= ring_limit


def ring_order(members):
    column = members // 4
    return [2 * i for i in range(column)] + [2 * i + 1 for i in reversed(range(column))]


def ring_gather(shard, axis):
    members = lax.axis_size(axis)
    order = ring_order(members)
    pairs = len(order)
    here = lax.axis_index(axis)
    parity = here % 2
    place = [0] * pairs
    for spot, pair in enumerate(order):
        place[pair] = spot
    spot_here = jnp.asarray(place, jnp.int32)[here // 2]
    order_table = jnp.asarray(order, jnp.int32)
    swap = [(i, i ^ 1) for i in range(members)]
    step = []
    for spot, pair in enumerate(order):
        step.append((2 * pair, 2 * order[(spot + 1) % pairs]))
        step.append((2 * pair + 1, 2 * order[(spot - 1) % pairs] + 1))
    way = 1 - 2 * parity

    def source_pair(hops, direction):
        return order_table[(spot_here - direction * hops + pairs) % pairs]

    found = [(here, shard)]
    mate = lax.ppermute(shard, axis, swap)
    found.append((here ^ 1, mate))
    own_stream, mate_stream = shard, mate
    for hops in range(1, pairs // 2 + 1):
        from_pair = source_pair(hops, way)
        other_pair = source_pair(hops, -way)
        own_stream = lax.ppermute(own_stream, axis, step)
        found.append((2 * from_pair + parity, own_stream))
        found.append((2 * other_pair + 1 - parity, lax.ppermute(own_stream, axis, swap)))
        if hops < pairs // 2:
            mate_stream = lax.ppermute(mate_stream, axis, step)
            found.append((2 * from_pair + 1 - parity, mate_stream))
            found.append((2 * other_pair + parity, lax.ppermute(mate_stream, axis, swap)))
    return found


def gather_rows(shard, axis):
    members = lax.axis_size(axis)
    if not use_ring(members):
        return lax.all_gather(shard, axis, axis=0, tiled=True)
    whole = jnp.zeros((members,) + shard.shape, shard.dtype)
    for position, piece in ring_gather(shard, axis):
        whole = lax.dynamic_update_slice(whole, piece[None], (position, 0, 0))
    return whole.reshape((-1,) + shard.shape[1:])


def on_device(
    tokens,
    segment_ids,
    expert_ids,
    attn_gain,
    sinks,
    qkv_master,
    qkv_mom,
    qkv_var,
    qkv_grad,
    o_master,
    o_mom,
    o_var,
    o_grad,
    router_weight,
    router_bias,
    mlp_gain,
):
    tok_rows = tokens.shape[0]
    width = tokens.shape[1]
    groups = lax.axis_size("dp")
    half_rows = tok_rows // groups
    group_index = lax.axis_index("dp")
    heads_here = sinks.shape[0]
    kv_here = KV_HEADS * heads_here // HEADS
    repeat_count = heads_here // kv_here
    q_rows = heads_here * HEAD_DIM
    kv_rows = kv_here * HEAD_DIM
    qkv_local = adam_weights(qkv_master, qkv_mom, qkv_var, qkv_grad)
    o_local = adam_weights(o_master, o_mom, o_var, o_grad)
    normed = rms_scale(tokens.astype(jnp.float32), attn_gain).astype(jnp.bfloat16)
    qkv_full = gather_rows(qkv_local, "expert")
    o_full = gather_rows(o_local, "expert")
    projected = lax.dot_general(normed, qkv_full, contract_rows, preferred_element_type=jnp.float32)
    positions = jnp.arange(tok_rows).astype(jnp.float32)
    queries = rotate(
        projected[:, :q_rows].reshape(tok_rows, heads_here, HEAD_DIM), positions
    ).astype(jnp.bfloat16)
    queries = queries.reshape(tok_rows, kv_here, repeat_count, HEAD_DIM)
    key_rows = rotate(
        projected[:, q_rows : q_rows + kv_rows].reshape(tok_rows, kv_here, HEAD_DIM), positions
    ).astype(jnp.bfloat16)
    value_rows = (
        projected[:, q_rows + kv_rows :].reshape(tok_rows, kv_here, HEAD_DIM).astype(jnp.bfloat16)
    )
    attended = attention(queries, key_rows, value_rows, segment_ids, sinks)
    own_rows = lax.dynamic_slice_in_dim(tokens, group_index * half_rows, half_rows, 0)
    own_choices = lax.dynamic_slice_in_dim(expert_ids, group_index * half_rows, half_rows, 0)
    if groups == 2:
        peer_rows = lax.dynamic_slice_in_dim(
            attended, (1 - group_index) * half_rows, half_rows, 0
        )
        mine = lax.dynamic_slice_in_dim(attended, group_index * half_rows, half_rows, 0)
        for_peer = jnp.dot(peer_rows, o_full, preferred_element_type=jnp.float32)
        arrived = lax.ppermute(for_peer.astype(jnp.bfloat16), "dp", [(0, 1), (1, 0)])
        summed = jnp.dot(mine, o_full, preferred_element_type=jnp.float32) + arrived.astype(
            jnp.float32
        )
    else:
        update = jnp.dot(attended, o_full, preferred_element_type=jnp.float32)
        summed = lax.psum_scatter(
            update.astype(jnp.bfloat16), "dp", scatter_dimension=0, tiled=True
        ).astype(jnp.float32)
    residual = own_rows.astype(jnp.float32) + summed
    moe_in = rms_scale(residual, mlp_gain).astype(jnp.bfloat16)
    logits = jnp.dot(moe_in, router_weight, preferred_element_type=jnp.float32) + router_bias
    experts = router_weight.shape[1]
    top_count = expert_ids.shape[1]
    capacity = 2 * half_rows * top_count // experts
    gate_vals = gate_values(logits, own_choices, experts)
    slots = slot_numbers(own_choices, experts)
    sources = lax.axis_size("expert")
    per_device = experts // sources
    if use_ring(sources) and per_device == 1 and experts <= 256 and capacity <= 256:
        return spread_tokens(moe_in, own_choices, slots, gate_vals, capacity)
    target = (own_choices * capacity + slots).reshape(-1)
    matches = target[None, :] == jnp.arange(experts * capacity, dtype=jnp.int32)[:, None]
    token_match = jnp.any(matches.reshape(experts * capacity, half_rows, top_count), axis=2).astype(
        jnp.bfloat16
    )
    payload = jnp.dot(token_match, moe_in, preferred_element_type=jnp.float32).astype(jnp.bfloat16)
    slot_gates = jnp.sum(jnp.where(matches, gate_vals.reshape(-1)[None, :], 0.0), axis=1).astype(
        jnp.bfloat16
    )
    outgoing = (payload.reshape(experts, capacity, width), slot_gates.reshape(experts, capacity))
    got_rows, got_gates = (
        lax.all_to_all(outgoing[0], "expert", split_axis=0, concat_axis=0, tiled=True),
        lax.all_to_all(outgoing[1], "expert", split_axis=0, concat_axis=0, tiled=True),
    )
    dispatched = jnp.transpose(
        got_rows.reshape(sources, per_device, capacity, width), (1, 0, 2, 3)
    )[:, :, None]
    gate_slots = jnp.transpose(got_gates.reshape(sources, per_device, capacity), (1, 0, 2))[
        :, :, None
    ]
    return (dispatched, gate_slots)


def spread_tokens(moe_in, choices, slots, gate_vals, capacity):
    width = moe_in.shape[1]
    top_count = choices.shape[1]
    members = lax.axis_size("expert")
    expert_here = lax.axis_index("expert").astype(jnp.float32)
    parcel = jnp.concatenate(
        [
            moe_in,
            choices.astype(jnp.bfloat16),
            slots.astype(jnp.bfloat16),
            gate_vals.astype(jnp.bfloat16),
        ],
        axis=1,
    )
    dispatched = jnp.zeros((members, capacity, width), jnp.bfloat16)
    gate_slots = jnp.zeros((members, capacity), jnp.bfloat16)
    slot_line = jnp.arange(capacity, dtype=jnp.float32)[:, None, None]
    for position, piece in ring_gather(parcel, "expert"):
        tail = piece[:, width:].astype(jnp.float32)
        ids = tail[:, :top_count]
        slot_of = jnp.where(ids == expert_here, tail[:, top_count : 2 * top_count], -1.0)
        hit = slot_of[None] == slot_line
        chosen = jnp.any(hit, axis=2).astype(jnp.bfloat16)
        gates = jnp.sum(jnp.where(hit, tail[None, :, 2 * top_count :], 0.0), axis=(1, 2))
        rows = jnp.dot(chosen, piece[:, :width], preferred_element_type=jnp.float32)
        dispatched = lax.dynamic_update_slice(
            dispatched, rows.astype(jnp.bfloat16)[None], (position, 0, 0)
        )
        gate_slots = lax.dynamic_update_slice(
            gate_slots, gates.astype(jnp.bfloat16)[None], (position, 0)
        )
    return dispatched[None, :, None], gate_slots[None, :, None]


def solution(mesh):
    return jax.shard_map(
        on_device,
        mesh=mesh,
        in_specs=(
            P("expert", None),
            P("expert"),
            P("expert", None),
            P(),
            P("dp"),
            P(("dp", "expert"), None),
            P(("dp", "expert"), None),
            P(("dp", "expert"), None),
            P(("dp", "expert"), None),
            P(("dp", "expert"), None),
            P(("dp", "expert"), None),
            P(("dp", "expert"), None),
            P(("dp", "expert"), None),
            P(),
            P(),
            P(),
        ),
        out_specs=(P("expert", None, "dp", None, None), P("expert", None, "dp", None)),
        check_vma=False,
    )
```

```python
import jax
import jax.numpy as jnp
from jax import lax
from jax.experimental import pallas as pl
from jax.sharding import PartitionSpec as P

HEADS = 32
KV_HEADS = 4
HEAD_DIM = 64
WINDOW = 128


beta_one = 0.9
beta_two = 0.999
adam_step = 100
learn_rate = 0.02
adam_eps = 1e-08
norm_eps = 1e-05
rope_base = 150000.0
contract_rows = (((1,), (1,)), ((), ()))
ring_limit = 16


def adam_weights(master, moment, second_mom, gradient):
    moment_new = beta_one * moment + (1.0 - beta_one) * gradient
    second_new = beta_two * second_mom + (1.0 - beta_two) * gradient * gradient
    fix_one = 1.0 - beta_one**adam_step
    fix_two = 1.0 - beta_two**adam_step
    update = moment_new / fix_one / (jnp.sqrt(second_new / fix_two) + adam_eps)
    return (master - learn_rate * update).astype(jnp.bfloat16)


def rms_scale(values, gain_vec):
    mean_sq = jnp.mean(values * values, axis=-1, keepdims=True)
    return values * lax.rsqrt(mean_sq + norm_eps) * gain_vec


def rotate(values, positions):
    half_dim = values.shape[-1] // 2
    frequency = rope_base ** (-(jnp.arange(half_dim).astype(jnp.float32) * 2.0) / values.shape[-1])
    angles = positions[:, None] * frequency[None, :]
    cosine = jnp.cos(angles)[:, None, :]
    sine_vals = jnp.sin(angles)[:, None, :]
    first_half = values[..., :half_dim]
    second_half = values[..., half_dim:]
    return jnp.concatenate(
        [
            first_half * cosine - second_half * sine_vals,
            second_half * cosine + first_half * sine_vals,
        ],
        axis=-1,
    )


def attention(queries, key_rows, value_rows, segments, sink_logits):
    row_count = queries.shape[0]
    scale = queries.shape[-1] ** (-0.5)
    scores = (
        jnp.einsum("tgrd,ugd->grtu", queries, key_rows, preferred_element_type=jnp.float32) * scale
    )
    position = jnp.arange(row_count, dtype=jnp.int32)
    offset = position[:, None] - position[None, :]
    allowed = (segments[:, None] == segments[None, :]) & (offset >= 0) & (offset < WINDOW)
    weights = jnp.where(allowed, jnp.exp(scores), 0.0)
    sink_terms = jnp.exp(sink_logits).reshape(key_rows.shape[1], -1)[:, :, None]
    running = sink_terms + jnp.sum(weights, axis=-1)
    attn_probs = (weights / running[..., None]).astype(jnp.bfloat16)
    attended = jnp.einsum(
        "grtu,ugd->tgrd", attn_probs, value_rows, preferred_element_type=jnp.float32
    )
    return attended.astype(jnp.bfloat16).reshape(row_count, -1)


def gate_values(logits, choices, experts):
    picked = choices[:, :, None] == jnp.arange(experts, dtype=jnp.int32)[None, None, :]
    chosen = jnp.sum(jnp.where(picked, logits[:, None, :], 0.0), axis=-1)
    raised = jnp.exp(chosen)
    return raised / jnp.sum(raised, axis=-1, keepdims=True)


def slot_numbers(choices, experts):
    flat_ids = choices.reshape(-1)
    onehot = (flat_ids[:, None] == jnp.arange(experts, dtype=jnp.int32)[None, :]).astype(jnp.int32)
    earlier = jnp.cumsum(onehot, axis=0) - onehot
    return jnp.sum(earlier * onehot, axis=1).reshape(choices.shape)


def use_ring(members):
    return members % 4 == 0 and members <= ring_limit


def ring_order(members):
    column = members // 4
    return [2 * i for i in range(column)] + [2 * i + 1 for i in reversed(range(column))]


def ring_gather(shard, axis, after=None):
    members = lax.axis_size(axis)
    order = ring_order(members)
    pairs = len(order)
    column = pairs // 2
    here = lax.axis_index(axis)
    parity = here & 1
    pair_here = here >> 1
    spot_here = jnp.where((pair_here & 1) == 1, pairs - 1 - (pair_here >> 1), pair_here >> 1)
    swap = [(i, i ^ 1) for i in range(members)]
    step = []
    for spot, pair in enumerate(order):
        step.append((2 * pair, 2 * order[(spot + 1) % pairs]))
        step.append((2 * pair + 1, 2 * order[(spot - 1) % pairs] + 1))

    def source_pair(shift):
        spot = spot_here + shift
        spot = jnp.where(spot >= pairs, spot - pairs, jnp.where(spot < 0, spot + pairs, spot))
        return jnp.where(spot < column, 2 * spot, 2 * (pairs - 1 - spot) + 1)

    def send(value, perm):
        return lax.ppermute(value, axis, perm)

    if after is not None:
        shard, _ = lax.optimization_barrier((shard, after))
    found = [(here, shard)]
    own_stream = send(shard, step)
    mate = send(shard, swap)
    found.append((here ^ 1, mate))
    mate_stream = mate
    mark = own_stream
    for hops in range(1, column + 1):
        behind = source_pair(-hops)
        ahead = source_pair(hops)
        from_pair = jnp.where(parity == 0, behind, ahead)
        other_pair = jnp.where(parity == 0, ahead, behind)
        if hops > 1:
            mark = own_stream
            own_stream = send(own_stream, step)
        found.append((2 * from_pair + parity, own_stream))
        found.append((2 * other_pair + 1 - parity, send(own_stream, swap)))
        if hops < column:
            mate_stream = send(mate_stream, step)
            found.append((2 * from_pair + 1 - parity, mate_stream))
            found.append((2 * other_pair + parity, send(mate_stream, swap)))
    return found, mark


def blank(shape, dtype):
    return pl.pallas_call(
        lambda out: None,
        out_shape=jax.ShapeDtypeStruct(shape, dtype),
        out_specs=pl.BlockSpec(memory_space=pl.ANY),
        name="blank",
    )()


def gather_rows(shard, axis, after=None):
    members = lax.axis_size(axis)
    if not use_ring(members):
        return lax.all_gather(shard, axis, axis=0, tiled=True), None
    whole = blank((members,) + shard.shape, shard.dtype)
    found, mark = ring_gather(shard, axis, after)
    for position, piece in found:
        whole = lax.dynamic_update_slice(whole, piece[None], (position, 0, 0))
    return whole.reshape((-1,) + shard.shape[1:]), mark


def layer(
    tokens,
    segment_ids,
    expert_ids,
    attn_gain,
    sinks,
    qkv_master,
    qkv_mom,
    qkv_var,
    qkv_grad,
    o_master,
    o_mom,
    o_var,
    o_grad,
    router_weight,
    router_bias,
    mlp_gain,
):
    tok_rows = tokens.shape[0]
    width = tokens.shape[1]
    groups = lax.axis_size("dp")
    half_rows = tok_rows // groups
    group_index = lax.axis_index("dp")
    heads_here = sinks.shape[0]
    kv_here = KV_HEADS * heads_here // HEADS
    repeat_count = heads_here // kv_here
    q_rows = heads_here * HEAD_DIM
    kv_rows = kv_here * HEAD_DIM
    qkv_local = adam_weights(qkv_master, qkv_mom, qkv_var, qkv_grad)
    o_local = adam_weights(o_master, o_mom, o_var, o_grad)
    normed = rms_scale(tokens.astype(jnp.float32), attn_gain).astype(jnp.bfloat16)
    own_rows = lax.dynamic_slice_in_dim(tokens, group_index * half_rows, half_rows, 0)
    qkv_full, mark = gather_rows(qkv_local, "expert")
    o_full, _ = gather_rows(o_local, "expert", mark)
    projected = lax.dot_general(normed, qkv_full, contract_rows, preferred_element_type=jnp.float32)
    positions = jnp.arange(tok_rows).astype(jnp.float32)
    queries = rotate(
        projected[:, :q_rows].reshape(tok_rows, heads_here, HEAD_DIM), positions
    ).astype(jnp.bfloat16)
    queries = queries.reshape(tok_rows, kv_here, repeat_count, HEAD_DIM)
    key_rows = rotate(
        projected[:, q_rows : q_rows + kv_rows].reshape(tok_rows, kv_here, HEAD_DIM), positions
    ).astype(jnp.bfloat16)
    value_rows = (
        projected[:, q_rows + kv_rows :].reshape(tok_rows, kv_here, HEAD_DIM).astype(jnp.bfloat16)
    )
    attended = attention(queries, key_rows, value_rows, segment_ids, sinks)
    own_choices = lax.dynamic_slice_in_dim(expert_ids, group_index * half_rows, half_rows, 0)
    if groups == 2:
        peer_rows = lax.dynamic_slice_in_dim(
            attended, (1 - group_index) * half_rows, half_rows, 0
        )
        mine = lax.dynamic_slice_in_dim(attended, group_index * half_rows, half_rows, 0)
        for_peer = jnp.dot(peer_rows, o_full, preferred_element_type=jnp.float32)
        arrived = lax.ppermute(for_peer.astype(jnp.bfloat16), "dp", [(0, 1), (1, 0)])
        local = own_rows.astype(jnp.float32) + jnp.dot(
            mine, o_full, preferred_element_type=jnp.float32
        )
        residual = lax.optimization_barrier(local) + arrived.astype(jnp.float32)
    else:
        update = jnp.dot(attended, o_full, preferred_element_type=jnp.float32)
        summed = lax.psum_scatter(
            update.astype(jnp.bfloat16), "dp", scatter_dimension=0, tiled=True
        ).astype(jnp.float32)
        residual = own_rows.astype(jnp.float32) + summed
    moe_in = rms_scale(residual, mlp_gain).astype(jnp.bfloat16)
    logits = jnp.dot(moe_in, router_weight, preferred_element_type=jnp.float32) + router_bias
    experts = router_weight.shape[1]
    top_count = expert_ids.shape[1]
    capacity = 2 * half_rows * top_count // experts
    gate_vals = gate_values(logits, own_choices, experts)
    slots = slot_numbers(own_choices, experts)
    sources = lax.axis_size("expert")
    per_device = experts // sources
    if use_ring(sources) and per_device == 1 and experts <= 256 and capacity <= 256:
        return spread_tokens(moe_in, own_choices, slots, gate_vals, capacity)
    target = (own_choices * capacity + slots).reshape(-1)
    matches = target[None, :] == jnp.arange(experts * capacity, dtype=jnp.int32)[:, None]
    token_match = jnp.any(matches.reshape(experts * capacity, half_rows, top_count), axis=2).astype(
        jnp.bfloat16
    )
    payload = jnp.dot(token_match, moe_in, preferred_element_type=jnp.float32).astype(jnp.bfloat16)
    slot_gates = jnp.sum(jnp.where(matches, gate_vals.reshape(-1)[None, :], 0.0), axis=1).astype(
        jnp.bfloat16
    )
    outgoing = (payload.reshape(experts, capacity, width), slot_gates.reshape(experts, capacity))
    got_rows, got_gates = (
        lax.all_to_all(outgoing[0], "expert", split_axis=0, concat_axis=0, tiled=True),
        lax.all_to_all(outgoing[1], "expert", split_axis=0, concat_axis=0, tiled=True),
    )
    dispatched = jnp.transpose(
        got_rows.reshape(sources, per_device, capacity, width), (1, 0, 2, 3)
    )[:, :, None]
    gate_slots = jnp.transpose(got_gates.reshape(sources, per_device, capacity), (1, 0, 2))[
        :, :, None
    ]
    return (dispatched, gate_slots)


def spread_tokens(moe_in, choices, slots, gate_vals, capacity):
    width = moe_in.shape[1]
    top_count = choices.shape[1]
    members = lax.axis_size("expert")
    expert_here = lax.axis_index("expert").astype(jnp.float32)
    parcel = jnp.concatenate(
        [
            moe_in,
            choices.astype(jnp.bfloat16),
            slots.astype(jnp.bfloat16),
            gate_vals.astype(jnp.bfloat16),
        ],
        axis=1,
    )
    dispatched = blank((members, capacity, width), jnp.bfloat16)
    gate_slots = jnp.zeros((members, capacity), jnp.bfloat16)
    slot_line = jnp.arange(capacity, dtype=jnp.float32)[:, None]
    for position, piece in ring_gather(parcel, "expert")[0]:
        tail = piece[:, width:].astype(jnp.float32).T
        chosen = jnp.zeros((capacity, piece.shape[0]), jnp.bool_)
        gates = jnp.zeros((capacity, piece.shape[0]), jnp.float32)
        for k in range(top_count):
            slot_of = jnp.where(tail[k] == expert_here, tail[top_count + k], -1.0)
            hit = slot_of[None, :] == slot_line
            chosen = chosen | hit
            gates = gates + jnp.where(hit, tail[2 * top_count + k][None, :], 0.0)
        rows = jnp.dot(
            chosen.astype(jnp.bfloat16), piece[:, :width], preferred_element_type=jnp.float32
        )
        dispatched = lax.dynamic_update_slice(
            dispatched, rows.astype(jnp.bfloat16)[None], (position, 0, 0)
        )
        gate_slots = lax.dynamic_update_slice(
            gate_slots, jnp.sum(gates, axis=1).astype(jnp.bfloat16)[None], (position, 0)
        )
    return dispatched[None, :, None], gate_slots[None, :, None]


def solution(mesh):
    return jax.shard_map(
        layer,
        mesh=mesh,
        in_specs=(
            P("expert", None),
            P("expert"),
            P("expert", None),
            P(),
            P("dp"),
            P(("dp", "expert"), None),
            P(("dp", "expert"), None),
            P(("dp", "expert"), None),
            P(("dp", "expert"), None),
            P(("dp", "expert"), None),
            P(("dp", "expert"), None),
            P(("dp", "expert"), None),
            P(("dp", "expert"), None),
            P(),
            P(),
            P(),
        ),
        out_specs=(P("expert", None, "dp", None, None), P("expert", None, "dp", None)),
        check_vma=False,
    )
```
